32 devices in a mesh: dp: 4 (over z), expert: 4 (over y, x), tensor: 2 (over core).
Axes of the slice: x: 2, y: 2, z: 4, core: 2. Of those that a mesh axis runs over, the one named last changes fastest.
Arguments:
- tokens: bfloat16 [512, 6144], P('dp', 'tensor'), may hold values from -6 to 6
- out_grad: bfloat16 [512, 6144], P('dp', 'tensor'), may hold values from -6 to 6
- router_weight: bfloat16 [6144, 4], P('tensor'), may hold values from -0.078125 to 0.078125
- gate_weight: bfloat16 [4, 6144, 8192], P('expert', 'tensor', 'dp'), may hold values from -0.078125 to 0.078125
- up_weight: bfloat16 [4, 6144, 8192], P('expert', 'tensor', 'dp'), may hold values from -0.078125 to 0.078125
- down_weight: bfloat16 [4, 8192, 6144], P('expert', 'dp', 'tensor'), may hold values from -0.0625 to 0.0625
- expert_index: int32 [512, 2], P('dp'), may hold values from 0 to 3, as said below
- slot_index: int32 [512, 2], P('dp'), may hold values from 0 to 95, as said below
Outputs:
- tokens_grad: bfloat16 [512, 6144], P(('dp', 'expert'), 'tensor')
- router_grad: float32 [6144, 4], P('tensor')
- gate_grad: bfloat16 [4, 6144, 8192], P('expert', 'tensor', 'dp')
- up_grad: bfloat16 [4, 6144, 8192], P('expert', 'tensor', 'dp')
- down_grad: bfloat16 [4, 8192, 6144], P('expert', 'dp', 'tensor')
The draws below stay inside these ranges and needn't reach their ends.
Inputs may be any that keep to these rules, and one draw needn't show every extreme that they name: `expert_index`: each row names two different experts; in each aligned block of 128 rows no expert is named more than 96 times, and one expert is named exactly 96 times in every block. `slot_index`: entry k of a row is a slot of the expert in entry k of the same row of expert_index; within one aligned block of 128 rows the choices of one expert have distinct slots.
All inputs are finite; a program needn't handle non-finite values.
Results may differ from the reference program's by a relative error of at most 0.025.
Values may be sent and summed in bfloat16 or wider, within the bound.
A program may use at most 128 MiB of HBM per device.

```python
from functools import partial
import jax
import jax.numpy as jnp
from jax import lax

D = 6144
FF = 8192
EXPERTS = 4
TOK_DEV = 128
CAP = 96
TOKENS = 512
SLOTS = 384
N_TENSOR = 2


def routing_block(block_key, busiest):
    load_key, order_key, token_key, swap_key, slot_key = jax.random.split(block_key, 5)
    shares = jax.random.randint(load_key, (EXPERTS - 1,), 1, 4)
    rest_picks = 2 * TOK_DEV - CAP
    other_loads = rest_picks * shares // jnp.sum(shares)
    leftover = rest_picks - jnp.sum(other_loads)
    other_loads = other_loads.at[jnp.argmin(shares)].add(leftover)
    others = (busiest + 1 + jax.random.permutation(order_key, EXPERTS - 1)) % EXPERTS
    expert_order = jnp.concatenate([jnp.reshape(busiest, (1,)), others]).astype(jnp.int32)
    run_counts = jnp.concatenate([jnp.array([CAP], jnp.int32), other_loads.astype(jnp.int32)])
    run_ends = jnp.cumsum(run_counts)
    run_starts = run_ends - run_counts
    pick_ids = jnp.arange(2 * TOK_DEV, dtype=jnp.int32)
    pick_run = jnp.sum((pick_ids[:, None] >= run_ends[None, :]).astype(jnp.int32), axis=1)
    pick_expert = expert_order[pick_run]
    pick_offset = pick_ids - run_starts[pick_run]
    tables = jax.vmap(partial(jax.random.permutation, x=CAP))(jax.random.split(slot_key, EXPERTS))
    pick_slot = tables[pick_expert, pick_offset]
    token_order = jax.random.permutation(token_key, TOK_DEV)
    first_pick = token_order
    second_pick = token_order + TOK_DEV
    expert_pair = jnp.stack([pick_expert[first_pick], pick_expert[second_pick]], axis=1)
    slot_pair = jnp.stack([pick_slot[first_pick], pick_slot[second_pick]], axis=1)
    swap_pair = jax.random.randint(swap_key, (TOK_DEV, 1), 0, 2) == 1
    expert_pair = jnp.where(swap_pair, expert_pair[:, ::-1], expert_pair)
    slot_pair = jnp.where(swap_pair, slot_pair[:, ::-1], slot_pair)
    return (expert_pair, slot_pair)


def make_routes(key):
    base_key = jax.random.fold_in(key, 7)
    row_blocks = TOKENS // TOK_DEV
    busiest = jax.random.randint(jax.random.fold_in(base_key, 1), (), 0, EXPERTS).astype(jnp.int32)
    block_keys = jax.random.split(jax.random.fold_in(base_key, 2), row_blocks)
    expert_pair, slot_pair = jax.vmap(partial(routing_block, busiest=busiest))(block_keys)
    return (expert_pair.reshape(TOKENS, 2).astype(jnp.int32), slot_pair.reshape(TOKENS, 2).astype(jnp.int32))


def draw_expert_index(key, part):
    return make_routes(key)[0]


def draw_slot_index(key, part):
    return make_routes(key)[1]


def shard_levels(stream_key, dims, cuts, smallest, largest):
    loudness = 1.0
    for position, parts in cuts:
        heights = jax.random.uniform(jax.random.fold_in(jax.random.fold_in(stream_key, 6), position), (parts,), jnp.float32, smallest / len(cuts), largest / len(cuts))
        loudness = loudness * jnp.repeat(jnp.exp(heights), dims[position] // parts).reshape((-1,) + (1,) * (len(dims) - 1 - position))
    return loudness


def normal_values(stream_key, dims, scale, reach, pieces=(), kind=jnp.bfloat16):
    entries = scale * jax.random.normal(stream_key, dims, jnp.float32)
    if pieces:
        entries = entries * shard_levels(stream_key, dims, pieces, -0.22, 0.18)
    return jnp.clip(entries, -reach, reach).astype(kind)


def setup_inputs(seed: int = 0) -> dict:
    key_list = jax.random.split(jax.random.key(seed), 9)
    tokens = normal_values(key_list[0], (TOKENS, D), 1.0, 6.0, ((0, 4), (1, 2)))
    out_grad = normal_values(key_list[1], (TOKENS, D), 1.0, 6.0, ((0, 4), (1, 2)))
    router_weight = normal_values(key_list[2], (D, EXPERTS), D ** -0.5, 0.078125, ((0, 2),))
    gate_weight = normal_values(key_list[3], (EXPERTS, D, FF), D ** -0.5, 0.078125, ((0, 4), (1, 2), (2, 4)))
    up_weight = normal_values(key_list[4], (EXPERTS, D, FF), D ** -0.5, 0.078125, ((0, 4), (1, 2), (2, 4)))
    down_weight = normal_values(key_list[5], (EXPERTS, FF, D), FF ** -0.5, 0.0625, ((0, 4), (1, 4), (2, 2)))
    expert_index = draw_expert_index(jax.random.fold_in(key_list[8], 71), 0)
    slot_index = draw_slot_index(jax.random.fold_in(key_list[8], 71), 0)
    return dict(tokens=tokens, out_grad=out_grad, router_weight=router_weight, gate_weight=gate_weight, up_weight=up_weight, down_weight=down_weight, expert_index=expert_index, slot_index=slot_index)


highest = lax.Precision.HIGHEST


def block_sum(left_side, right_side):
    block_width = D // N_TENSOR
    running = jnp.zeros((left_side.shape[0], right_side.shape[1]), jnp.float32)
    for row_block in range(N_TENSOR):
        partial_value = jnp.dot(left_side[:, row_block * block_width:(row_block + 1) * block_width], right_side[row_block * block_width:(row_block + 1) * block_width], preferred_element_type=jnp.float32)
        partial_value = lax.optimization_barrier(partial_value.astype(jnp.bfloat16)).astype(jnp.float32)
        running = running + partial_value
    return running


def expert_backward(operands):
    slot_tokens, slot_grads, slot_prob, gate_w, up_w, down_w = operands
    gate_sum = block_sum(slot_tokens, gate_w)
    up_sum = block_sum(slot_tokens, up_w)
    grad_act = block_sum(slot_grads, down_w.T)
    gate_sigmoid = jax.nn.sigmoid(gate_sum)
    hidden = (gate_sum * gate_sigmoid * up_sum).astype(jnp.bfloat16)
    prob_grad = jnp.sum(hidden.astype(jnp.float32) * grad_act, axis=1)
    act_grad = slot_prob.astype(jnp.float32)[:, None] * grad_act
    grad_gate = (act_grad * up_sum * gate_sigmoid * (1.0 + gate_sum * (1.0 - gate_sigmoid))).astype(jnp.bfloat16)
    grad_up = (act_grad * gate_sum * gate_sigmoid).astype(jnp.bfloat16)
    scaled_grads = (slot_prob.astype(jnp.float32)[:, None] * slot_grads.astype(jnp.float32)).astype(jnp.bfloat16)
    down_grad = jnp.dot(hidden.T, scaled_grads, preferred_element_type=jnp.float32).astype(jnp.bfloat16)
    gate_grad = jnp.dot(slot_tokens.T, grad_gate, preferred_element_type=jnp.float32).astype(jnp.bfloat16)
    up_grad = jnp.dot(slot_tokens.T, grad_up, preferred_element_type=jnp.float32).astype(jnp.bfloat16)
    slot_dx = jnp.dot(grad_gate, gate_w.T, preferred_element_type=jnp.float32) + jnp.dot(grad_up, up_w.T, preferred_element_type=jnp.float32)
    return slot_dx, prob_grad, gate_grad, up_grad, down_grad


def reference(tokens, out_grad, router_weight, gate_weight, up_weight, down_weight, expert_index, slot_index):
    logits = jnp.dot(tokens, router_weight, preferred_element_type=jnp.float32)
    chosen = jnp.take_along_axis(logits, expert_index, axis=1)
    pick_prob = jnp.stack([jax.nn.sigmoid(chosen[:, 0] - chosen[:, 1]), jax.nn.sigmoid(chosen[:, 1] - chosen[:, 0])], axis=1)
    prob_low = pick_prob.astype(jnp.bfloat16)
    row_block = (jnp.arange(TOKENS, dtype=jnp.int32) // TOK_DEV).astype(jnp.int32)
    slot_place = ((expert_index * (TOKENS // TOK_DEV) + row_block[:, None]) * CAP + slot_index).astype(jnp.int32)
    flat_place = slot_place.reshape(-1)
    slot_tokens = jnp.zeros((EXPERTS * SLOTS, D), jnp.bfloat16).at[flat_place].set(jnp.repeat(tokens, 2, axis=0))
    slot_grads = jnp.zeros((EXPERTS * SLOTS, D), jnp.bfloat16).at[flat_place].set(jnp.repeat(out_grad, 2, axis=0))
    slot_prob = jnp.zeros((EXPERTS * SLOTS,), jnp.bfloat16).at[flat_place].set(prob_low.reshape(-1))
    slot_dx, prob_grad, gate_grad, up_grad, down_grad = lax.map(expert_backward, (slot_tokens.reshape(EXPERTS, SLOTS, D), slot_grads.reshape(EXPERTS, SLOTS, D), slot_prob.reshape(EXPERTS, SLOTS), gate_weight, up_weight, down_weight))
    pick_dx = slot_dx.reshape(EXPERTS * SLOTS, D)[slot_place]
    pick_grad = prob_grad.reshape(-1)[slot_place]
    mixed_grad = jnp.sum(pick_prob * pick_grad, axis=1, keepdims=True)
    weights = pick_prob * (pick_grad - mixed_grad)
    onehot = (expert_index[:, :, None] == jnp.arange(EXPERTS, dtype=jnp.int32)[None, None, :]).astype(jnp.float32)
    logit_grad = jnp.sum(onehot * weights[:, :, None], axis=1)
    tokens_grad = (jnp.sum(pick_dx, axis=1) + jnp.dot(logit_grad, router_weight.astype(jnp.float32).T, precision=highest)).astype(jnp.bfloat16)
    router_grad = jnp.dot(tokens.astype(jnp.float32).T, logit_grad, precision=highest)
    return tokens_grad, router_grad, gate_grad, up_grad, down_grad
```

```python
import jax
import jax.numpy as jnp
from jax import lax
from jax.sharding import PartitionSpec as P

CAP = 96
F32 = jnp.float32
BF16 = jnp.bfloat16


def contract_rows(left_side, right_side):
    return lax.dot_general(
        left_side, right_side, (((0,), (0,)), ((), ())), preferred_element_type=F32
    )


def contract_cols(left_side, right_side):
    return lax.dot_general(
        left_side, right_side, (((1,), (1,)), ((), ())), preferred_element_type=F32
    )


def build(n_dp, n_exp, n_ten):
    def dp_shift(values, step):
        return lax.ppermute(values, "dp", [(i, (i + step) % n_dp) for i in range(n_dp)])

    def exp_swap(values, mask):
        return lax.ppermute(values, "expert", [(i, i ^ mask) for i in range(n_exp)])

    def ten_sum(values):
        total = values.astype(F32)
        for step in range(1, n_ten):
            perm = [(i, (i + step) % n_ten) for i in range(n_ten)]
            total = total + lax.ppermute(values, "tensor", perm).astype(F32)
        return total

    def spread_expert(rows):
        if n_exp != 4:
            return [rows] + [exp_swap(rows, j) for j in range(1, n_exp)]
        from_x = exp_swap(rows, 1)
        from_y = exp_swap(rows, 2)
        half = rows.shape[0] // 2
        first = exp_swap(from_x[:half], 2)
        second = exp_swap(from_y[half:], 1)
        return [rows, from_x, from_y, jnp.concatenate([first, second], axis=0)]

    def reduce_expert(parts):
        if n_exp != 4:
            total = parts[0].astype(F32)
            for j in range(1, n_exp):
                total = total + exp_swap(parts[j], j).astype(F32)
            return total
        half = parts[0].shape[0] // 2

        def two_steps(view, near, far):
            got_own = exp_swap(view(parts[near]), near)
            got_far = exp_swap(view(parts[3]), near)
            relay = (view(parts[far]).astype(F32) + got_far.astype(F32)).astype(BF16)
            got_relay = exp_swap(relay, far)
            return view(parts[0]).astype(F32) + got_own.astype(F32) + got_relay.astype(F32)

        top = two_steps(lambda v: v[:half], 1, 2)
        low = two_steps(lambda v: v[half:], 2, 1)
        return jnp.concatenate([top, low], axis=0)

    def shards(
        tokens, out_grad, router_weight, gate_weight, up_weight, down_weight, expert_index, slot_index
    ):
        cap = CAP
        rows, width = tokens.shape
        n_choice = router_weight.shape[1]
        quarter = rows // n_exp
        expert_id = lax.axis_index("expert")
        dp_id = lax.axis_index("dp")

        def own_quarter(values, mask):
            return lax.dynamic_slice_in_dim(values, (expert_id ^ mask) * quarter, quarter, 0)

        def by_mask(values):
            return jnp.concatenate([own_quarter(values, j) for j in range(n_exp)], axis=0)

        def gather_z(values):
            mine = own_quarter(values, 0)
            return [dp_shift(mine, k) for k in range(1, n_dp)]

        def gather_plane(values, remote):
            spread = spread_expert(jnp.concatenate(remote, axis=0))
            stacked = jnp.stack([s.reshape(n_dp - 1, quarter, width) for s in spread], axis=1)
            stacked = stacked.reshape(n_dp - 1, rows, width)
            return jnp.concatenate([by_mask(values)[None], stacked], axis=0)

        tokens_z = gather_z(tokens)
        index_own = jnp.concatenate([expert_index, slot_index], axis=1).T
        index_all = jnp.stack(
            [index_own] + [dp_shift(index_own, k) for k in range(1, n_dp)], axis=0
        )
        grads_z = gather_z(out_grad)
        tokens_all = gather_plane(tokens, tokens_z)
        grads_all = gather_plane(out_grad, grads_z)

        index_all = jnp.concatenate(
            [
                lax.dynamic_slice_in_dim(index_all, (expert_id ^ j) * quarter, quarter, 2)
                for j in range(n_exp)
            ],
            axis=2,
        )
        pick = [index_all[:, 0], index_all[:, 1]]
        place = [index_all[:, 2], index_all[:, 3]]
        positions = lax.broadcasted_iota(jnp.int32, (n_dp, cap, rows), 1)
        tables = [
            (pick[k] == expert_id)[:, None, :] & (place[k][:, None, :] == positions)
            for k in range(2)
        ]
        select = (tables[0] | tables[1]).astype(BF16)

        def to_slots(values):
            out = jnp.einsum("kcn,knd->kcd", select, values, preferred_element_type=F32)
            return out.astype(BF16).reshape(n_dp * cap, width)

        gate_block = gate_weight[0]
        up_block = up_weight[0]
        down_block = down_weight[0]

        slot_tokens = to_slots(tokens_all)
        gate_part = jnp.dot(slot_tokens, gate_block, preferred_element_type=F32).astype(BF16)
        gate_sum = ten_sum(gate_part)
        logits_part = lax.dot_general(
            router_weight,
            tokens_all.reshape(n_dp * rows, width),
            (((0,), (1,)), ((), ())),
            preferred_element_type=F32,
        )
        logits = ten_sum(logits_part).reshape(n_choice, n_dp, rows)
        up_part = jnp.dot(slot_tokens, up_block, preferred_element_type=F32).astype(BF16)
        up_sum = ten_sum(up_part)
        slot_grads = to_slots(grads_all)
        grad_part = contract_cols(slot_grads, down_block).astype(BF16)
        grad_sum = ten_sum(grad_part)

        choice_ids = lax.broadcasted_iota(jnp.int32, (n_choice, n_dp, rows), 0)
        chosen = [jnp.sum(jnp.where(choice_ids == pick[k][None], logits, 0.0), axis=0) for k in range(2)]
        prob = [jax.nn.sigmoid(chosen[0] - chosen[1]), jax.nn.sigmoid(chosen[1] - chosen[0])]

        def to_slot_vec(first, second):
            picked = jnp.where(tables[0], first[:, None, :], 0.0) + jnp.where(
                tables[1], second[:, None, :], 0.0
            )
            return jnp.sum(picked, axis=2).reshape(n_dp * cap)

        low = [p.astype(BF16).astype(F32) for p in prob]
        slot_prob = to_slot_vec(low[0], low[1])[:, None]

        gate_sigmoid = jax.nn.sigmoid(gate_sum)
        hidden = (gate_sum * gate_sigmoid * up_sum).astype(BF16)
        prob_grad = jnp.sum(hidden.astype(F32) * grad_sum, axis=1)
        act_grad = slot_prob * grad_sum
        grad_gate = (
            act_grad * up_sum * gate_sigmoid * (1.0 + gate_sum * (1.0 - gate_sigmoid))
        ).astype(BF16)
        grad_up = (act_grad * gate_sum * gate_sigmoid).astype(BF16)
        hidden, grad_gate, grad_up = lax.optimization_barrier((hidden, grad_gate, grad_up))
        scaled_grads = (slot_prob * slot_grads.astype(F32)).astype(BF16)

        prob_grad = prob_grad.reshape(n_dp, cap)
        part_sum = prob_grad
        for k in range(1, n_dp):
            got = dp_shift(prob_grad, k)
            part_sum = part_sum + jnp.roll(got, k, axis=0)
        tables_by_mask = [part_sum] + [exp_swap(part_sum, j) for j in range(1, n_exp)]
        expert_tables = jnp.stack(tables_by_mask, axis=0)
        mask_ids = lax.broadcasted_iota(jnp.int32, (n_exp, n_dp, rows), 0) ^ expert_id
        slot_ids = lax.broadcasted_iota(jnp.int32, (n_dp, cap, rows), 1)
        pick_grad = []
        for k in range(2):
            at_slot = place[k][:, None, :] == slot_ids
            per_exp = jnp.stack(
                [
                    jnp.sum(jnp.where(at_slot, expert_tables[j][:, :, None], 0.0), axis=1)
                    for j in range(n_exp)
                ],
                axis=0,
            )
            pick_grad.append(jnp.sum(jnp.where(mask_ids == pick[k][None], per_exp, 0.0), axis=0))
        mixed = prob[0] * pick_grad[0] + prob[1] * pick_grad[1]
        weights = [prob[k] * (pick_grad[k] - mixed) for k in range(2)]

        chunks = 2 if width % 256 == 0 else 1
        step = width // chunks
        dx_parts = []
        for c in range(chunks):
            cols = slice(c * step, (c + 1) * step)
            slot_dx = contract_cols(grad_gate, gate_block[cols]) + contract_cols(
                grad_up, up_block[cols]
            )
            slot_dx = slot_dx.astype(BF16).reshape(n_dp, cap, step)
            token_dx = jnp.einsum(
                "kcn,kcd->knd", select, slot_dx, preferred_element_type=F32
            ).astype(BF16)
            token_dx = token_dx.reshape(n_dp, n_exp, quarter, step)
            summed = reduce_expert([token_dx[:, j] for j in range(n_exp)])
            total = summed[0]
            for k in range(1, n_dp):
                total = total + dp_shift(summed[(-k) % n_dp].astype(BF16), k).astype(F32)
            dx_parts.append(total)

        gate_grad = contract_rows(slot_tokens, grad_gate).astype(BF16)
        up_grad = contract_rows(slot_tokens, grad_up).astype(BF16)
        down_grad = contract_rows(hidden, scaled_grads).astype(BF16)

        slot_logit = to_slot_vec(weights[0], weights[1])
        high = slot_logit.astype(BF16)
        rest = slot_logit - high.astype(F32)
        middle = rest.astype(BF16)
        final = (rest - middle.astype(F32)).astype(BF16)
        column = jnp.sum(
            lax.dot_general(
                jnp.stack([high, middle, final], axis=0),
                slot_tokens,
                (((1,), (0,)), ((), ())),
                preferred_element_type=F32,
            ),
            axis=0,
            keepdims=True,
        )
        columns = jnp.concatenate([column] + [exp_swap(column, j) for j in range(1, n_exp)], axis=0)
        out_rows = lax.broadcasted_iota(jnp.int32, (n_choice, 1), 0)
        router_grad = jnp.zeros((n_choice, width), F32)
        for j in range(n_exp):
            router_grad = router_grad + jnp.where(out_rows == (expert_id ^ j), columns[j : j + 1], 0.0)
        router_grad = router_grad.T

        near = lax.broadcasted_iota(jnp.int32, (quarter, n_choice), 1)
        logit_grad = sum(
            jnp.where(near == pick[k][0, :quarter][:, None], weights[k][0, :quarter][:, None], 0.0)
            for k in range(2)
        )
        router_term = jnp.dot(
            logit_grad, router_weight.astype(F32).T, precision=lax.Precision.HIGHEST
        )
        tokens_grad = (jnp.concatenate(dx_parts, axis=1) + router_term).astype(BF16)
        return (tokens_grad, router_grad, gate_grad[None], up_grad[None], down_grad[None])

    return shards


def solution(mesh):
    in_specs = (
        P("dp", "tensor"),
        P("dp", "tensor"),
        P("tensor", None),
        P("expert", "tensor", "dp"),
        P("expert", "tensor", "dp"),
        P("expert", "dp", "tensor"),
        P("dp", None),
        P("dp", None),
    )
    out_specs = (
        P(("dp", "expert"), "tensor"),
        P("tensor", None),
        P("expert", "tensor", "dp"),
        P("expert", "tensor", "dp"),
        P("expert", "dp", "tensor"),
    )
    shards = build(mesh.shape["dp"], mesh.shape["expert"], mesh.shape["tensor"])
    return jax.shard_map(shards, mesh=mesh, in_specs=in_specs, out_specs=out_specs, check_vma=False)
```

```python
import jax
import jax.numpy as jnp
from jax import lax
from jax.sharding import PartitionSpec as P

CAP = 96
F32 = jnp.float32
BF16 = jnp.bfloat16


def contract_rows(left_side, right_side):
    return lax.dot_general(
        left_side, right_side, (((0,), (0,)), ((), ())), preferred_element_type=F32
    )


def contract_cols(left_side, right_side):
    return lax.dot_general(
        left_side, right_side, (((1,), (1,)), ((), ())), preferred_element_type=F32
    )


def build(n_dp, n_exp, n_ten):
    def dp_shift(values, step):
        return lax.ppermute(values, "dp", [(i, (i + step) % n_dp) for i in range(n_dp)])

    def exp_swap(values, mask):
        return lax.ppermute(values, "expert", [(i, i ^ mask) for i in range(n_exp)])

    def ten_sum(values):
        total = values.astype(F32)
        for step in range(1, n_ten):
            perm = [(i, (i + step) % n_ten) for i in range(n_ten)]
            total = total + lax.ppermute(values, "tensor", perm).astype(F32)
        return total

    def spread_expert(rows):
        if n_exp != 4:
            return [rows] + [exp_swap(rows, j) for j in range(1, n_exp)]
        from_x = exp_swap(rows, 1)
        from_y = exp_swap(rows, 2)
        half = rows.shape[0] // 2
        first = exp_swap(from_x[:half], 2)
        second = exp_swap(from_y[half:], 1)
        return [rows, from_x, from_y, jnp.concatenate([first, second], axis=0)]

    def double_expert(values):
        stack, mask = values[None], 1
        while mask < n_exp:
            stack = jnp.concatenate([stack, exp_swap(stack, mask)], axis=0)
            mask *= 2
        return stack

    def reduce_first(parts):
        if n_exp != 4:
            return [exp_swap(parts[j], j) for j in range(1, n_exp)]
        half = parts[0].shape[0] // 2
        return [
            exp_swap(jnp.stack([parts[1][:half], parts[3][:half]]), 1),
            exp_swap(jnp.stack([parts[2][half:], parts[3][half:]]), 2),
        ]

    def reduce_relay(parts, got):
        if n_exp != 4:
            return []
        half = parts[0].shape[0] // 2
        top = (parts[2][:half].astype(F32) + got[0][1].astype(F32)).astype(BF16)
        low = (parts[1][half:].astype(F32) + got[1][1].astype(F32)).astype(BF16)
        return [exp_swap(top, 2), exp_swap(low, 1)]

    def reduce_last(parts, got, relayed):
        own = parts[0].astype(F32)
        if n_exp != 4:
            for piece in got:
                own = own + piece.astype(F32)
            return own
        half = parts[0].shape[0] // 2
        top = own[:half] + got[0][0].astype(F32) + relayed[0].astype(F32)
        low = own[half:] + got[1][0].astype(F32) + relayed[1].astype(F32)
        return jnp.concatenate([top, low], axis=0)

    def shards(
        tokens, out_grad, router_weight, gate_weight, up_weight, down_weight, expert_index, slot_index
    ):
        cap = CAP
        rows, width = tokens.shape
        n_choice = router_weight.shape[1]
        quarter = rows // n_exp
        expert_id = lax.axis_index("expert")
        dp_id = lax.axis_index("dp")

        def own_quarter(values, mask):
            return lax.dynamic_slice_in_dim(values, (expert_id ^ mask) * quarter, quarter, 0)

        def by_mask(values):
            return jnp.concatenate([own_quarter(values, j) for j in range(n_exp)], axis=0)

        def gather_z(values):
            mine = own_quarter(values, 0)
            return [dp_shift(mine, k) for k in range(1, n_dp)]

        def gather_plane(values, remote):
            spread = spread_expert(jnp.concatenate(remote, axis=0))
            stacked = jnp.stack([s.reshape(n_dp - 1, quarter, width) for s in spread], axis=1)
            stacked = stacked.reshape(n_dp - 1, rows, width)
            return jnp.concatenate([by_mask(values)[None], stacked], axis=0)

        index_own = jnp.concatenate([expert_index, slot_index], axis=1).T
        tokens_z = gather_z(tokens)
        tokens_z, out_grad, index_own = lax.optimization_barrier((tokens_z, out_grad, index_own))
        grads_z = gather_z(out_grad)
        index_all = jnp.stack(
            [index_own] + [dp_shift(index_own, k) for k in range(1, n_dp)], axis=0
        )
        tokens_all = gather_plane(tokens, tokens_z)
        grads_all = gather_plane(out_grad, grads_z)

        index_all = jnp.concatenate(
            [
                lax.dynamic_slice_in_dim(index_all, (expert_id ^ j) * quarter, quarter, 2)
                for j in range(n_exp)
            ],
            axis=2,
        )
        pick = [index_all[:, 0], index_all[:, 1]]
        place = [index_all[:, 2], index_all[:, 3]]
        positions = lax.broadcasted_iota(jnp.int32, (n_dp, cap, rows), 1)
        tables = [
            (pick[k] == expert_id)[:, None, :] & (place[k][:, None, :] == positions)
            for k in range(2)
        ]
        select = (tables[0] | tables[1]).astype(BF16)

        def to_slots(values):
            out = jnp.einsum("kcn,knd->kcd", select, values, preferred_element_type=F32)
            return out.astype(BF16).reshape(n_dp * cap, width)

        gate_block = gate_weight[0]
        up_block = up_weight[0]
        down_block = down_weight[0]

        slot_tokens = to_slots(tokens_all)
        gate_part = jnp.dot(slot_tokens, gate_block, preferred_element_type=F32).astype(BF16)
        gate_sum = ten_sum(gate_part)
        logits_part = lax.dot_general(
            router_weight,
            tokens_all.reshape(n_dp * rows, width),
            (((0,), (1,)), ((), ())),
            preferred_element_type=F32,
        )
        logits = ten_sum(logits_part).reshape(n_choice, n_dp, rows)
        up_part = jnp.dot(slot_tokens, up_block, preferred_element_type=F32).astype(BF16)
        grads_all, up_part = lax.optimization_barrier((grads_all, up_part))
        slot_grads = to_slots(grads_all)
        grad_part = contract_cols(slot_grads, down_block).astype(BF16)
        up_sum = ten_sum(up_part)
        grad_sum = ten_sum(grad_part)

        choice_ids = lax.broadcasted_iota(jnp.int32, (n_choice, n_dp, rows), 0)
        chosen = [jnp.sum(jnp.where(choice_ids == pick[k][None], logits, 0.0), axis=0) for k in range(2)]
        prob = [jax.nn.sigmoid(chosen[0] - chosen[1]), jax.nn.sigmoid(chosen[1] - chosen[0])]

        def to_slot_vec(first, second):
            picked = jnp.where(tables[0], first[:, None, :], 0.0) + jnp.where(
                tables[1], second[:, None, :], 0.0
            )
            return jnp.sum(picked, axis=2).reshape(n_dp * cap)

        low = [p.astype(BF16).astype(F32) for p in prob]
        slot_prob = to_slot_vec(low[0], low[1])[:, None]

        gate_sigmoid = jax.nn.sigmoid(gate_sum)
        hidden = (gate_sum * gate_sigmoid * up_sum).astype(BF16)
        prob_grad = jnp.sum(hidden.astype(F32) * grad_sum, axis=1)
        act_grad = slot_prob * grad_sum
        grad_gate = (
            act_grad * up_sum * gate_sigmoid * (1.0 + gate_sum * (1.0 - gate_sigmoid))
        ).astype(BF16)
        grad_up = (act_grad * gate_sum * gate_sigmoid).astype(BF16)
        hidden, grad_gate, grad_up = lax.optimization_barrier((hidden, grad_gate, grad_up))
        scaled_grads = (slot_prob * slot_grads.astype(F32)).astype(BF16)

        chunks = 2 if width % 256 == 0 else 1
        step = width // chunks
        parts, got = [], []
        gate_in, up_in = grad_gate, grad_up
        for c in range(chunks):
            cols = slice(c * step, (c + 1) * step)
            slot_dx = contract_cols(gate_in, gate_block[cols]) + contract_cols(up_in, up_block[cols])
            slot_dx = slot_dx.astype(BF16).reshape(n_dp, cap, step)
            token_dx = jnp.einsum(
                "kcn,kcd->knd", select, slot_dx, preferred_element_type=F32
            ).astype(BF16)
            token_dx, gate_in, up_in = lax.optimization_barrier((token_dx, gate_in, up_in))
            token_dx = token_dx.reshape(n_dp, n_exp, quarter, step)
            parts.append([token_dx[:, j] for j in range(n_exp)])
            got.append(reduce_first(parts[c]))

        def over_dp(summed):
            return [dp_shift(summed[(-k) % n_dp].astype(BF16), k) for k in range(1, n_dp)]

        last = chunks - 1
        prob_grad, gate_in, hidden = lax.optimization_barrier((prob_grad, gate_in, hidden))
        relayed, summed, crossed = [None] * chunks, [None] * chunks, [None] * chunks
        if chunks == 2:
            relayed[0] = reduce_relay(parts[0], got[0])
        gate_grad = contract_rows(slot_tokens, gate_in).astype(BF16)
        gate_grad, up_in, got[last], relayed[0] = lax.optimization_barrier(
            (gate_grad, up_in, got[last], relayed[0])
        )
        relayed[last] = reduce_relay(parts[last], got[last])
        if chunks == 2:
            summed[0] = reduce_last(parts[0], got[0], relayed[0])
            crossed[0] = over_dp(summed[0])
        up_grad = contract_rows(slot_tokens, up_in).astype(BF16)
        up_grad, hidden, relayed[last], crossed[0] = lax.optimization_barrier(
            (up_grad, hidden, relayed[last], crossed[0])
        )
        summed[last] = reduce_last(parts[last], got[last], relayed[last])
        crossed[last] = over_dp(summed[last])
        down_grad = contract_rows(hidden, scaled_grads).astype(BF16)
        dx_parts = []
        for c in range(chunks):
            total = summed[c][0]
            for piece in crossed[c]:
                total = total + piece.astype(F32)
            dx_parts.append(total)

        prob_grad = prob_grad.reshape(n_dp, cap)
        part_sum = prob_grad
        for k in range(1, n_dp):
            got = dp_shift(prob_grad, k)
            part_sum = part_sum + jnp.roll(got, k, axis=0)
        expert_tables = double_expert(part_sum)
        mask_ids = lax.broadcasted_iota(jnp.int32, (n_exp, n_dp, rows), 0) ^ expert_id
        slot_ids = lax.broadcasted_iota(jnp.int32, (n_dp, cap, rows), 1)
        pick_grad = []
        for k in range(2):
            at_slot = place[k][:, None, :] == slot_ids
            per_exp = jnp.stack(
                [
                    jnp.sum(jnp.where(at_slot, expert_tables[j][:, :, None], 0.0), axis=1)
                    for j in range(n_exp)
                ],
                axis=0,
            )
            pick_grad.append(jnp.sum(jnp.where(mask_ids == pick[k][None], per_exp, 0.0), axis=0))
        mixed = prob[0] * pick_grad[0] + prob[1] * pick_grad[1]
        weights = [prob[k] * (pick_grad[k] - mixed) for k in range(2)]

        slot_logit = to_slot_vec(weights[0], weights[1])
        high = slot_logit.astype(BF16)
        rest = slot_logit - high.astype(F32)
        middle = rest.astype(BF16)
        final = (rest - middle.astype(F32)).astype(BF16)
        column = jnp.sum(
            lax.dot_general(
                jnp.stack([high, middle, final], axis=0),
                slot_tokens,
                (((1,), (0,)), ((), ())),
                preferred_element_type=F32,
            ),
            axis=0,
            keepdims=True,
        )
        columns = double_expert(column[0])
        out_rows = lax.broadcasted_iota(jnp.int32, (n_choice, 1), 0)
        router_grad = jnp.zeros((n_choice, width), F32)
        for j in range(n_exp):
            router_grad = router_grad + jnp.where(out_rows == (expert_id ^ j), columns[j : j + 1], 0.0)
        router_grad = router_grad.T

        near = lax.broadcasted_iota(jnp.int32, (quarter, n_choice), 1)
        logit_grad = sum(
            jnp.where(near == pick[k][0, :quarter][:, None], weights[k][0, :quarter][:, None], 0.0)
            for k in range(2)
        )
        router_term = jnp.dot(
            logit_grad, router_weight.astype(F32).T, precision=lax.Precision.HIGHEST
        )
        tokens_grad = (jnp.concatenate(dx_parts, axis=1) + router_term).astype(BF16)
        return (tokens_grad, router_grad, gate_grad[None], up_grad[None], down_grad[None])

    return shards


def solution(mesh):
    in_specs = (
        P("dp", "tensor"),
        P("dp", "tensor"),
        P("tensor", None),
        P("expert", "tensor", "dp"),
        P("expert", "tensor", "dp"),
        P("expert", "dp", "tensor"),
        P("dp", None),
        P("dp", None),
    )
    out_specs = (
        P(("dp", "expert"), "tensor"),
        P("tensor", None),
        P("expert", "tensor", "dp"),
        P("expert", "tensor", "dp"),
        P("expert", "dp", "tensor"),
    )
    shards = build(mesh.shape["dp"], mesh.shape["expert"], mesh.shape["tensor"])
    return jax.shard_map(shards, mesh=mesh, in_specs=in_specs, out_specs=out_specs, check_vma=False)
```
